32 devices in a mesh: mom: 8 (over y, x, core), en: 4 (over z).
Axes of the slice: x: 2, y: 2, z: 4, core: 2. Of those that a mesh axis runs over, the one named last changes fastest.
Arguments:
- green: bfloat16 [2, 8, 16, 2, 128, 128], P(None, 'mom', 'en'), may hold values from -0.5 to 0.5
- bare: bfloat16 [2, 8, 16, 2, 128, 128], P(None, 'mom', 'en'), may hold values from -0.5 to 0.5
- coupling: bfloat16 [4, 128, 128], replicated, may hold values from -0.25 to 0.25
- occupation: float32 [4], replicated, may hold values from 0.2 to 2
- mode_shift: int32 [4], replicated, may hold values from -1 to 1, as said below
- mode_offset: int32 [4], replicated, may hold values from 1 to 4, as said below
- mode_block: int32 [2, 4], replicated, may hold values from 0 to 1
Outputs:
- updated: bfloat16 [2, 8, 16, 2, 128, 128], P(None, 'mom', 'en')
The draws below stay inside these ranges and needn't reach their ends.
Inputs may be any that keep to these rules, and one draw needn't show every extreme that they name: `mode_shift`: each of -1, 0 and 1 is the shift of some mode. `mode_offset`: every offset from 1 to 4 is some mode's.
All inputs are finite; a program needn't handle non-finite values.
Results may differ from the reference program's by a relative error of at most 0.02.
Values may be sent and summed in bfloat16 or wider, within the bound.
A program may use at most 64 MiB of HBM per device.

```python
import math
import jax
import jax.numpy as jnp
from jax import lax

ORBITALS = 128
BLOCKS = 2
MODES = 4
REACH = 4
PASSES = 2
MOMENTA = 8
ENERGIES = 16


def draw_mode_shift(key, part):
    order = jax.random.permutation(jax.random.fold_in(key, 11), MODES)
    return (order % 3 - 1).astype(jnp.int32)


def draw_mode_offset(key, part):
    order = jax.random.permutation(jax.random.fold_in(key, 23), MODES)
    return (order % REACH + 1).astype(jnp.int32)


def plant(entries, own_key, least, high):
    dims = entries.shape
    place = [jax.random.randint(jax.random.fold_in(own_key, axis), (), 0, dims[axis]) for axis in range(len(dims))]
    entries = entries.at[tuple(place)].set(least)
    longest = dims.index(max(dims))
    place[longest] = (place[longest] + 1) % dims[longest]
    return entries.at[tuple(place)].set(high)


def block_scale(key, extent, split, low, largest):
    def one(position, shards_of):
        steps = jax.random.uniform(jax.random.fold_in(jax.random.fold_in(key, 6), position), (shards_of,), jnp.float32, low / len(split), largest / len(split))
        return jnp.repeat(jnp.exp(steps), extent[position] // shards_of).reshape((-1,) + (1,) * (len(extent) - position - 1))

    gain = one(*split[0])
    for cut in split[1:]:
        gain = gain * one(*cut)
    return gain


def noise(key, shape, width, limit, split=(), kind=jnp.bfloat16):
    array = width * jax.random.normal(key, shape, jnp.float32)
    if split:
        array = array * block_scale(key, shape, split, -0.22, 0.18)
    return jnp.clip(array, -limit, limit).astype(kind)


def setup_inputs(seed: int = 0) -> dict:
    streams_of = jax.random.split(jax.random.key(seed), 8)
    return {
        "green": noise(streams_of[0], (2, MOMENTA, ENERGIES, BLOCKS, ORBITALS, ORBITALS), ORBITALS ** -0.5, 0.5, ((1, 8), (2, 4))),
        "bare": noise(streams_of[1], (2, MOMENTA, ENERGIES, BLOCKS, ORBITALS, ORBITALS), ORBITALS ** -0.5, 0.5, ((1, 8), (2, 4))),
        "coupling": noise(streams_of[2], (MODES, ORBITALS, ORBITALS), (4 * ORBITALS) ** -0.5, 0.25),
        "occupation": jnp.clip(jnp.exp(jax.random.uniform(streams_of[3], (MODES,), jnp.float32, math.log(0.2), math.log(2.0))), 0.2, 2.0),
        "mode_shift": draw_mode_shift(jax.random.fold_in(streams_of[7], 71), 0),
        "mode_offset": draw_mode_offset(jax.random.fold_in(streams_of[7], 71), 0),
        "mode_block": plant(jax.random.randint(streams_of[6], (BLOCKS, MODES), 0, BLOCKS), jax.random.fold_in(streams_of[6], 1), 0, BLOCKS - 1).astype(jnp.int32),
    }


def complex_product(left_pair, right_pair):
    left_float = left_pair.astype(jnp.float32)
    right_float = right_pair.astype(jnp.float32)
    real_part = jnp.einsum("...ab,...bc->...ac", left_float[0], right_float[0]) - jnp.einsum("...ab,...bc->...ac", left_float[1], right_float[1])
    imag_part = jnp.einsum("...ab,...bc->...ac", left_float[0], right_float[1]) + jnp.einsum("...ab,...bc->...ac", left_float[1], right_float[0])
    return jnp.stack([real_part, imag_part])


def one_point(padded, bare, coupling, occupation, mode_shift, mode_offset, mode_block, kpoint):
    summed_terms = jnp.zeros((2, ENERGIES, BLOCKS, ORBITALS, ORBITALS), jnp.float32)

    def add_mode(mode_index, accum):
        source_index = ((kpoint - mode_shift[mode_index]) % MOMENTA).astype(jnp.int32)
        source = lax.dynamic_index_in_dim(padded, source_index, 1, keepdims=False)
        lower_side = lax.dynamic_slice_in_dim(source, (REACH - mode_offset[mode_index]).astype(jnp.int32), ENERGIES, 1)
        upper_side = lax.dynamic_slice_in_dim(source, (REACH + mode_offset[mode_index]).astype(jnp.int32), ENERGIES, 1)
        lower_side = jnp.take(lower_side, mode_block[:, mode_index], axis=2)
        upper_side = jnp.take(upper_side, mode_block[:, mode_index], axis=2)
        weight = occupation[mode_index]
        summed = (weight * lower_side.astype(jnp.float32) + (weight + 1.0) * upper_side.astype(jnp.float32)).astype(jnp.bfloat16)
        matrix = coupling[mode_index].astype(jnp.float32)
        coupled = jnp.einsum("ab,...bc->...ac", matrix, summed.astype(jnp.float32)).astype(jnp.bfloat16)
        contribution = jnp.einsum("...ab,cb->...ac", coupled.astype(jnp.float32), matrix)
        return accum + contribution

    sigma = lax.fori_loop(0, MODES, add_mode, summed_terms).astype(jnp.bfloat16)
    bare_point = lax.dynamic_index_in_dim(bare, kpoint, 1, keepdims=False)
    product = complex_product(bare_point, sigma).astype(jnp.bfloat16)
    correction = complex_product(product, bare_point)
    return (bare_point.astype(jnp.float32) + correction).astype(jnp.bfloat16)


def reference(green, bare, coupling, occupation, mode_shift, mode_offset, mode_block):
    current = green
    for pass_index in range(PASSES):
        padded = jnp.pad(current, ((0, 0), (0, 0), (REACH, REACH), (0, 0), (0, 0), (0, 0)))
        points = lax.map(lambda kpoint: one_point(padded, bare, coupling, occupation, mode_shift, mode_offset, mode_block, kpoint), jnp.arange(MOMENTA, dtype=jnp.int32))
        current = jnp.moveaxis(points, 0, 1)
    return current
```

```python
import functools

import jax
import jax.numpy as jnp
from jax import lax
from jax.experimental import pallas as pl
from jax.experimental.pallas import tpu as pltpu
from jax.sharding import PartitionSpec as P

MODES = 4
REACH = 4
PASSES = 2

RAW_UP, RAW_DOWN, RAW_NEXT, RAW_PREV, SHARE_NEXT, SHARE_PREV, PART_UP, PART_DOWN = range(8)
KINDS = 8

f32 = jnp.float32
bf16 = jnp.bfloat16


def matmul(left, right):
    return jnp.dot(left, right, preferred_element_type=f32)


def side_by_side(*parts):
    return parts[0] if len(parts) == 1 else jnp.concatenate(parts, axis=1)


def on_top(*parts):
    return parts[0] if len(parts) == 1 else jnp.concatenate(parts, axis=0)


def kernel(
    mom_count, en_count, passes,
    occupation, mode_shift, mode_offset, mode_block, green, bare, coupling,
    out,
    matrices, matrices_t, pair_t, wide_bare, real_coupled, below, above,
    share_own, part_own, real_current, low_rim, high_rim, imag_source,
    share_out, share_in, part_out, part_in, send_sem, recv_sem,
):
    energies = green.shape[2]
    blocks = green.shape[3]
    size = green.shape[4]
    k = lax.axis_index("mom")
    z = lax.axis_index("en")
    next_k = lax.rem(k + 1, mom_count)
    prev_k = lax.rem(k + mom_count - 1, mom_count)
    up_z = lax.rem(z + 1, en_count)
    down_z = lax.rem(z + en_count - 1, en_count)
    has_up = z < en_count - 1
    has_down = z > 0

    barrier = pltpu.get_barrier_semaphore()
    for other in (next_k, prev_k):
        pl.semaphore_signal(
            barrier, inc=1, device_id={"mom": other}, device_id_type=pl.DeviceIdType.MESH
        )

    @pl.when(has_up)
    def _():
        pl.semaphore_signal(
            barrier, inc=1, device_id={"en": up_z}, device_id_type=pl.DeviceIdType.MESH
        )

    @pl.when(has_down)
    def _():
        pl.semaphore_signal(
            barrier, inc=1, device_id={"en": down_z}, device_id_type=pl.DeviceIdType.MESH
        )

    pl.semaphore_wait(barrier, 2 + has_up.astype(jnp.int32) + has_down.astype(jnp.int32))

    def copy_of(p, kind, e):
        if kind == RAW_UP or kind == RAW_DOWN:
            source = green.at[0, 0, e] if p == 0 else real_current[p - 1][e]
            target = low_rim[p][e] if kind == RAW_UP else high_rim[p][e]
        elif kind == RAW_NEXT or kind == RAW_PREV:
            source = green.at[1, 0, e] if p == 0 else imag_source[p][e].at[1]
            target = imag_source[p][e].at[2 if kind == RAW_NEXT else 0]
        elif kind == SHARE_NEXT or kind == SHARE_PREV:
            way = 1 if kind == SHARE_NEXT else 0
            source, target = share_out[p].at[way, e], share_in[p].at[way, e]
        else:
            way = 1 if kind == PART_UP else 0
            source, target = part_out[p].at[way, e], part_in[p].at[way, e]
        if kind in (RAW_NEXT, SHARE_NEXT):
            device = {"mom": next_k}
        elif kind in (RAW_PREV, SHARE_PREV):
            device = {"mom": prev_k}
        elif kind in (RAW_UP, PART_UP):
            device = {"en": up_z}
        else:
            device = {"en": down_z}
        return pltpu.make_async_remote_copy(
            src_ref=source,
            dst_ref=target,
            send_sem=send_sem.at[p, kind, e],
            recv_sem=recv_sem.at[p, kind, e],
            device_id=device,
            device_id_type=pl.DeviceIdType.MESH,
        )

    def guarded(condition, action):
        if condition is None:
            action()
        else:
            pl.when(condition)(action)

    def sends_if(kind):
        return {RAW_UP: has_up, PART_UP: has_up, RAW_DOWN: has_down, PART_DOWN: has_down}.get(kind)

    def receives_if(kind):
        return {RAW_UP: has_down, PART_UP: has_down, RAW_DOWN: has_up, PART_DOWN: has_up}.get(kind)

    def start(p, kind, e):
        guarded(sends_if(kind), lambda: copy_of(p, kind, e).start())

    waited = set()

    def arrived(p, kind, e):
        if (p, kind, e) not in waited:
            waited.add((p, kind, e))
            guarded(receives_if(kind), lambda: copy_of(p, kind, e).wait_recv())

    order = []
    for i in range((energies + 1) // 2):
        order.append(i)
        if energies - 1 - i != i:
            order.append(energies - 1 - i)

    for e in order:
        start(0, RAW_NEXT, e)
        start(0, RAW_PREV, e)
        start(0, RAW_UP, e)
        start(0, RAW_DOWN, e)

    @pl.when(jnp.logical_not(has_down))
    def _():
        for p in range(passes):
            for e in range(energies):
                low_rim[p][e][...] = jnp.zeros_like(low_rim[p][e])
            part_in[p][1] = jnp.zeros_like(part_in[p][1])

    @pl.when(jnp.logical_not(has_up))
    def _():
        for p in range(passes):
            for e in range(energies):
                high_rim[p][e][...] = jnp.zeros_like(high_rim[p][e])
            part_in[p][0] = jnp.zeros_like(part_in[p][0])

    weight, shift, picks = [], [], []
    for m in range(MODES):
        mode = jnp.int32(0)
        for j in range(1, MODES):
            mode = jnp.where(mode_offset[j] == m + 1, jnp.int32(j), mode)
        weight.append(occupation[mode])
        shift.append(mode_shift[mode])
        picks.append([mode_block[b, mode] for b in range(blocks)])
        matrix = coupling[mode]
        matrices[m] = matrix
        matrices_t[pl.ds(m * size, size), :] = matrix.astype(f32).T.astype(bf16)
    slot_of = []
    for q in (-1, 0, 1):
        slot = jnp.int32(0)
        for m in range(1, MODES):
            slot = jnp.where(shift[m] == q, jnp.int32(m), slot)
        slot_of.append(slot)
    extra = sum(range(MODES)) - slot_of[0] - slot_of[1] - slot_of[2]
    extra_shift = jnp.int32(0)
    for m in range(MODES):
        extra_shift = jnp.where(extra == m, shift[m], extra_shift)
    extra_t = matrices[extra].astype(f32).T
    for q in range(3):
        pair_t[q, pl.ds(0, size), :] = matrices[slot_of[q]].astype(f32).T.astype(bf16)
        kept = jnp.where(extra_shift == q - 1, 1.0, 0.0).astype(f32)
        pair_t[q, pl.ds(size, size), :] = (extra_t * kept).astype(bf16)

    for e in range(energies):
        for b in range(blocks):
            real, imag = bare[0, 0, e, b], bare[1, 0, e, b]
            wide_bare[e, b, pl.ds(0, size), :] = side_by_side(real, imag)
            wide_bare[e, b, pl.ds(size, size), :] = side_by_side(-imag, real)
        imag_source[0][e][1] = green[1, 0, e]

    def real_at(p, e, pick):
        if e < 0:
            return low_rim[p][e + energies][pick]
        if e >= energies:
            return high_rim[p][e - energies][pick]
        return green[0, 0, e, pick] if p == 0 else real_current[p - 1][e][pick]

    def imag_step(p, e):
        arrived(p, RAW_NEXT, e)
        arrived(p, RAW_PREV, e)
        for m in range(MODES):
            chosen = imag_source[p][e][shift[m] + 1]
            coupled = matmul(matrices[m], side_by_side(*[chosen[c] for c in range(blocks)]))
            lower = (weight[m] * coupled).astype(bf16)
            upper = ((weight[m] + 1.0) * coupled).astype(bf16)
            for c in range(blocks):
                below[e, m, c] = lower[:, c * size:(c + 1) * size]
                above[e, m, c] = upper[:, c * size:(c + 1) * size]

    def part_of(target):
        lower = [m for m in range(MODES) if 0 <= target - m - 1 < energies]
        upper = [m for m in range(MODES) if 0 <= target + m + 1 < energies]
        rows = []
        for b in range(blocks):
            terms = [below[target - m - 1, m, picks[m][b]] for m in lower]
            terms += [above[target + m + 1, m, picks[m][b]] for m in upper]
            rows.append(side_by_side(*terms))
        spans = [
            matrices_t[pl.ds(ms[0] * size, len(ms) * size), :] for ms in (lower, upper) if ms
        ]
        return matmul(on_top(*rows), on_top(*spans))

    def send_part(p, way, e):
        target = e + energies if way == 1 else e - energies
        part = part_of(target).astype(bf16)
        for b in range(blocks):
            part_out[p][way, e, b] = part[b * size:(b + 1) * size]
        start(p, PART_UP if way == 1 else PART_DOWN, e)

    def real_step(p, e):
        for m in range(MODES):
            for at in (e - m - 1, e + m + 1):
                if at < 0:
                    arrived(p, RAW_UP, at + energies)
                elif at >= energies:
                    arrived(p, RAW_DOWN, at - energies)
        for m in range(MODES):
            summed = []
            for b in range(blocks):
                low_side = real_at(p, e - m - 1, picks[m][b]).astype(f32)
                high_side = real_at(p, e + m + 1, picks[m][b]).astype(f32)
                mixed = weight[m] * low_side + (weight[m] + 1.0) * high_side
                summed.append(mixed.astype(bf16))
            coupled = matmul(matrices[m], side_by_side(*summed)).astype(bf16)
            for b in range(blocks):
                real_coupled[e, m, pl.ds(b * size, size), :] = coupled[:, b * size:(b + 1) * size]
        rest = real_coupled[e, extra]
        for q in (0, 2, 1):
            share = matmul(side_by_side(real_coupled[e, slot_of[q]], rest), pair_t[q])
            if q == 1:
                share_own[e] = share
            else:
                rounded = share.astype(bf16)
                way = 1 if q == 2 else 0
                for b in range(blocks):
                    share_out[p][way, e, b] = rounded[b * size:(b + 1) * size]
                start(p, SHARE_NEXT if way == 1 else SHARE_PREV, e)

    def close_step(p, e):
        for kind in (SHARE_NEXT, SHARE_PREV, PART_UP, PART_DOWN):
            arrived(p, kind, e)
        for b in range(blocks):
            rows = slice(b * size, (b + 1) * size)
            real = share_own[e, rows] + share_in[p][0, e, b].astype(f32)
            real = (real + share_in[p][1, e, b].astype(f32)).astype(bf16)
            imag = part_own[e, rows] + part_in[p][0, e, b].astype(f32)
            imag = (imag + part_in[p][1, e, b].astype(f32)).astype(bf16)
            sigma = on_top(side_by_side(real, imag), side_by_side(-imag, real))
            both = wide_bare[e, b, pl.ds(0, size), :]
            product = matmul(both, sigma).astype(bf16)
            new = (both.astype(f32) + matmul(product, wide_bare[e, b])).astype(bf16)
            if p == passes - 1:
                out[0, 0, e, b] = new[:, :size]
                out[1, 0, e, b] = new[:, size:]
            else:
                real_current[p][e][b] = new[:, :size]
                imag_source[p + 1][e][1, b] = new[:, size:]
        if p < passes - 1:
            start(p + 1, RAW_NEXT, e)
            start(p + 1, RAW_PREV, e)
            start(p + 1, RAW_UP, e)
            start(p + 1, RAW_DOWN, e)

    for p in range(passes):
        done = set()
        todo = []
        for e in order:
            imag_step(p, e)
            done.add(e)
            if len(done) < energies:
                if all(i in done for i in range(e + 1)):
                    send_part(p, 0, e)
                    todo.append((0, e))
                if all(i in done for i in range(e, energies)):
                    send_part(p, 1, e)
                    todo.append((1, e))
        rest = [
            (way, e)
            for i in range(energies)
            for way, e in ((0, i), (1, energies - 1 - i))
            if (way, e) not in todo
        ]
        inner = order[::-1]
        for i in range(energies):
            real_step(p, inner[i])
            share_of = rest[i * len(rest) // energies:(i + 1) * len(rest) // energies]
            for way, e in share_of:
                send_part(p, way, e)
        for e in order:
            part_own[e] = part_of(e)
        for e in inner:
            close_step(p, e)

    for p in range(passes):
        for kind in range(KINDS):
            def finish(p=p, kind=kind):
                for e in range(energies):
                    copy_of(p, kind, e).wait_send()

            guarded(sends_if(kind), finish)


def shards(mom_count, en_count, green, bare, coupling, occupation, mode_shift, mode_offset, mode_block):
    _, _, energies, blocks, size, _ = green.shape
    assert energies == REACH and coupling.shape[0] == MODES and MODES == REACH
    pair = (blocks, size, size)
    vmem = pltpu.VMEM
    scratch = [
        vmem((MODES, size, size), bf16),
        vmem((MODES * size, size), bf16),
        vmem((3, 2 * size, size), bf16),
        vmem((energies, blocks, 2 * size, 2 * size), bf16),
        vmem((energies, MODES, blocks * size, size), bf16),
        vmem((energies, MODES) + pair, bf16),
        vmem((energies, MODES) + pair, bf16),
        vmem((energies, blocks * size, size), f32),
        vmem((energies, blocks * size, size), f32),
        [[vmem(pair, bf16) for _ in range(energies)] for _ in range(PASSES - 1)],
        [[vmem(pair, bf16) for _ in range(energies)] for _ in range(PASSES)],
        [[vmem(pair, bf16) for _ in range(energies)] for _ in range(PASSES)],
        [[vmem((3,) + pair, bf16) for _ in range(energies)] for _ in range(PASSES)],
        [vmem((2, energies) + pair, bf16) for _ in range(PASSES)],
        [vmem((2, energies) + pair, bf16) for _ in range(PASSES)],
        [vmem((2, energies) + pair, bf16) for _ in range(PASSES)],
        [vmem((2, energies) + pair, bf16) for _ in range(PASSES)],
        pltpu.SemaphoreType.DMA((PASSES, KINDS, energies)),
        pltpu.SemaphoreType.DMA((PASSES, KINDS, energies)),
    ]
    whole = pl.BlockSpec(memory_space=pltpu.VMEM)
    scalars = pl.BlockSpec(memory_space=pltpu.SMEM)
    return pl.pallas_call(
        functools.partial(kernel, mom_count, en_count, PASSES),
        out_shape=jax.ShapeDtypeStruct(green.shape, green.dtype),
        in_specs=[scalars] * 4 + [whole] * 3,
        out_specs=whole,
        scratch_shapes=scratch,
        compiler_params=pltpu.CompilerParams(
            collective_id=0, has_side_effects=True, vmem_limit_bytes=48 * 1024 * 1024
        ),
        name="born_passes",
    )(occupation, mode_shift, mode_offset, mode_block, green, bare, coupling)


def solution(mesh):
    spread = P(None, "mom", "en", None, None, None)
    return jax.shard_map(
        functools.partial(shards, mesh.shape["mom"], mesh.shape["en"]),
        mesh=mesh,
        in_specs=(spread, spread, P(), P(), P(), P(), P()),
        out_specs=spread,
        check_vma=False,
    )
```

```python
import functools

import jax
import jax.numpy as jnp
from jax import lax
from jax.experimental import pallas as pl
from jax.experimental.pallas import tpu as pltpu
from jax.sharding import PartitionSpec as P

MODES = 4
REACH = 4
PASSES = 2

RAW_UP, RAW_DOWN, RAW_NEXT, RAW_PREV, SHARE_NEXT, SHARE_PREV, PART_UP, PART_DOWN = range(8)
KINDS = 8

f32 = jnp.float32
bf16 = jnp.bfloat16


def matmul(left, right):
    return jnp.dot(left, right, preferred_element_type=f32)


def side_by_side(*parts):
    return parts[0] if len(parts) == 1 else jnp.concatenate(parts, axis=1)


def on_top(*parts):
    return parts[0] if len(parts) == 1 else jnp.concatenate(parts, axis=0)


def kernel(
    mom_count, en_count, passes,
    occupation_hbm, mode_shift_hbm, mode_offset_hbm, mode_block_hbm, green, bare_hbm, coupling_hbm,
    out,
    occupation, mode_shift, mode_offset, mode_block, bare, coupling, first_real,
    matrices, matrices_t, pair_t, wide_bare, real_coupled, below, above,
    share_own, part_own, real_current, low_rim, high_rim, imag_source,
    share_out, share_in, part_out, part_in, send_sem, recv_sem, green_sem, input_sem,
):
    energies = green.shape[2]
    blocks = green.shape[3]
    size = green.shape[4]
    k = lax.axis_index("mom")
    z = lax.axis_index("en")
    next_k = lax.rem(k + 1, mom_count)
    prev_k = lax.rem(k + mom_count - 1, mom_count)
    up_z = lax.rem(z + 1, en_count)
    down_z = lax.rem(z + en_count - 1, en_count)
    has_up = z < en_count - 1
    has_down = z > 0

    barrier = pltpu.get_barrier_semaphore()
    for other in (next_k, prev_k):
        pl.semaphore_signal(
            barrier, inc=1, device_id={"mom": other}, device_id_type=pl.DeviceIdType.MESH
        )

    @pl.when(has_up)
    def _():
        pl.semaphore_signal(
            barrier, inc=1, device_id={"en": up_z}, device_id_type=pl.DeviceIdType.MESH
        )

    @pl.when(has_down)
    def _():
        pl.semaphore_signal(
            barrier, inc=1, device_id={"en": down_z}, device_id_type=pl.DeviceIdType.MESH
        )

    middle = list(range(1, energies - 1))
    ends = [0, energies - 1]
    upward = list(range(energies))[::-1]
    downward = list(range(energies))

    real_fetch = [
        pltpu.make_async_copy(green.at[0, 0, e], first_real[e], green_sem.at[0, e])
        for e in range(energies)
    ]
    imag_fetch = [
        pltpu.make_async_copy(green.at[1, 0, e], imag_source[0][e].at[1], green_sem.at[1, e])
        for e in range(energies)
    ]
    pairs = (
        (coupling_hbm, coupling),
        (bare_hbm, bare),
        (occupation_hbm, occupation),
        (mode_shift_hbm, mode_shift),
        (mode_offset_hbm, mode_offset),
        (mode_block_hbm, mode_block),
    )
    input_fetch = [
        pltpu.make_async_copy(there, here, input_sem.at[i]) for i, (there, here) in enumerate(pairs)
    ]
    for e in ends + middle:
        imag_fetch[e].start()
        real_fetch[e].start()
    for fetch in input_fetch:
        fetch.start()

    pl.semaphore_wait(barrier, 2 + has_up.astype(jnp.int32) + has_down.astype(jnp.int32))

    def copy_of(p, kind, e):
        if kind == RAW_UP or kind == RAW_DOWN:
            source = first_real[e] if p == 0 else real_current[p - 1][e]
            target = low_rim[p][e] if kind == RAW_UP else high_rim[p][e]
        elif kind == RAW_NEXT or kind == RAW_PREV:
            source = imag_source[p][e].at[1]
            target = imag_source[p][e].at[2 if kind == RAW_NEXT else 0]
        elif kind == SHARE_NEXT or kind == SHARE_PREV:
            way = 1 if kind == SHARE_NEXT else 0
            source, target = share_out[p].at[way, e], share_in[p].at[way, e]
        else:
            way = 1 if kind == PART_UP else 0
            source, target = part_out[p].at[way, e], part_in[p].at[way, e]
        if kind in (RAW_NEXT, SHARE_NEXT):
            device = {"mom": next_k}
        elif kind in (RAW_PREV, SHARE_PREV):
            device = {"mom": prev_k}
        elif kind in (RAW_UP, PART_UP):
            device = {"en": up_z}
        else:
            device = {"en": down_z}
        return pltpu.make_async_remote_copy(
            src_ref=source,
            dst_ref=target,
            send_sem=send_sem.at[p, kind, e],
            recv_sem=recv_sem.at[p, kind, e],
            device_id=device,
            device_id_type=pl.DeviceIdType.MESH,
        )

    def guarded(condition, action):
        if condition is None:
            action()
        else:
            pl.when(condition)(action)

    def sends_if(kind):
        return {RAW_UP: has_up, PART_UP: has_up, RAW_DOWN: has_down, PART_DOWN: has_down}.get(kind)

    def receives_if(kind):
        return {RAW_UP: has_down, PART_UP: has_down, RAW_DOWN: has_up, PART_DOWN: has_up}.get(kind)

    def start(p, kind, e):
        guarded(sends_if(kind), lambda: copy_of(p, kind, e).start())

    waited = set()

    def arrived(p, kind, e):
        if (p, kind, e) not in waited:
            waited.add((p, kind, e))
            guarded(receives_if(kind), lambda: copy_of(p, kind, e).wait_recv())

    for i, e in enumerate(ends + middle):
        imag_fetch[e].wait()
        start(0, RAW_NEXT, e)
        start(0, RAW_PREV, e)
    for fetch in real_fetch:
        fetch.wait()
    for i in range(energies):
        start(0, RAW_UP, upward[i])
        start(0, RAW_DOWN, downward[i])

    @pl.when(jnp.logical_not(has_down))
    def _():
        for p in range(passes):
            for e in range(energies):
                low_rim[p][e][...] = jnp.zeros_like(low_rim[p][e])
            part_in[p][1] = jnp.zeros_like(part_in[p][1])

    @pl.when(jnp.logical_not(has_up))
    def _():
        for p in range(passes):
            for e in range(energies):
                high_rim[p][e][...] = jnp.zeros_like(high_rim[p][e])
            part_in[p][0] = jnp.zeros_like(part_in[p][0])

    for fetch in input_fetch:
        fetch.wait()

    weight, shift, picks = [], [], []
    for m in range(MODES):
        mode = jnp.int32(0)
        for j in range(1, MODES):
            mode = jnp.where(mode_offset[j] == m + 1, jnp.int32(j), mode)
        weight.append(occupation[mode])
        shift.append(mode_shift[mode])
        picks.append([mode_block[b, mode] for b in range(blocks)])
        matrix = coupling[mode]
        matrices[m] = matrix
        matrices_t[pl.ds(m * size, size), :] = matrix.astype(f32).T.astype(bf16)
    slot_of = []
    for q in (-1, 0, 1):
        slot = jnp.int32(0)
        for m in range(1, MODES):
            slot = jnp.where(shift[m] == q, jnp.int32(m), slot)
        slot_of.append(slot)
    extra = sum(range(MODES)) - slot_of[0] - slot_of[1] - slot_of[2]
    extra_shift = jnp.int32(0)
    for m in range(MODES):
        extra_shift = jnp.where(extra == m, shift[m], extra_shift)
    extra_t = matrices[extra].astype(f32).T
    for q in range(3):
        pair_t[q, pl.ds(0, size), :] = matrices[slot_of[q]].astype(f32).T.astype(bf16)
        kept = jnp.where(extra_shift == q - 1, 1.0, 0.0).astype(f32)
        pair_t[q, pl.ds(size, size), :] = (extra_t * kept).astype(bf16)

    for e in range(energies):
        for b in range(blocks):
            real, imag = bare[0, 0, e, b], bare[1, 0, e, b]
            wide_bare[e, b, pl.ds(0, size), :] = side_by_side(real, imag)
            wide_bare[e, b, pl.ds(size, size), :] = side_by_side(-imag, real)

    def real_at(p, e, pick):
        if e < 0:
            return low_rim[p][e + energies][pick]
        if e >= energies:
            return high_rim[p][e - energies][pick]
        return first_real[e][pick] if p == 0 else real_current[p - 1][e][pick]

    def imag_step(p, e):
        arrived(p, RAW_NEXT, e)
        arrived(p, RAW_PREV, e)
        for m in range(MODES):
            chosen = imag_source[p][e][shift[m] + 1]
            coupled = matmul(matrices[m], side_by_side(*[chosen[c] for c in range(blocks)]))
            lower = (weight[m] * coupled).astype(bf16)
            upper = ((weight[m] + 1.0) * coupled).astype(bf16)
            for c in range(blocks):
                below[e, m, c] = lower[:, c * size:(c + 1) * size]
                above[e, m, c] = upper[:, c * size:(c + 1) * size]

    def part_of(target):
        lower = [m for m in range(MODES) if 0 <= target - m - 1 < energies]
        upper = [m for m in range(MODES) if 0 <= target + m + 1 < energies]
        rows = []
        for b in range(blocks):
            terms = [below[target - m - 1, m, picks[m][b]] for m in lower]
            terms += [above[target + m + 1, m, picks[m][b]] for m in upper]
            rows.append(side_by_side(*terms))
        spans = [
            matrices_t[pl.ds(ms[0] * size, len(ms) * size), :] for ms in (lower, upper) if ms
        ]
        return matmul(on_top(*rows), on_top(*spans))

    def send_part(p, way, e):
        target = e + energies if way == 1 else e - energies
        part = part_of(target).astype(bf16)
        for b in range(blocks):
            part_out[p][way, e, b] = part[b * size:(b + 1) * size]
        start(p, PART_UP if way == 1 else PART_DOWN, e)

    def real_step(p, e):
        for m in range(MODES):
            for at in (e - m - 1, e + m + 1):
                if at < 0:
                    arrived(p, RAW_UP, at + energies)
                elif at >= energies:
                    arrived(p, RAW_DOWN, at - energies)
        for m in range(MODES):
            summed = []
            for b in range(blocks):
                low_side = real_at(p, e - m - 1, picks[m][b]).astype(f32)
                high_side = real_at(p, e + m + 1, picks[m][b]).astype(f32)
                mixed = weight[m] * low_side + (weight[m] + 1.0) * high_side
                summed.append(mixed.astype(bf16))
            coupled = matmul(matrices[m], side_by_side(*summed)).astype(bf16)
            for b in range(blocks):
                real_coupled[e, m, pl.ds(b * size, size), :] = coupled[:, b * size:(b + 1) * size]
        rest = real_coupled[e, extra]
        for q in (0, 2, 1):
            share = matmul(side_by_side(real_coupled[e, slot_of[q]], rest), pair_t[q])
            if q == 1:
                share_own[e] = share
            else:
                rounded = share.astype(bf16)
                way = 1 if q == 2 else 0
                for b in range(blocks):
                    share_out[p][way, e, b] = rounded[b * size:(b + 1) * size]
                start(p, SHARE_NEXT if way == 1 else SHARE_PREV, e)

    def close_step(p, e):
        for kind in (SHARE_NEXT, SHARE_PREV, PART_UP, PART_DOWN):
            arrived(p, kind, e)
        for b in range(blocks):
            rows = slice(b * size, (b + 1) * size)
            real = share_own[e, rows] + share_in[p][0, e, b].astype(f32)
            real = (real + share_in[p][1, e, b].astype(f32)).astype(bf16)
            imag = part_own[e, rows] + part_in[p][0, e, b].astype(f32)
            imag = (imag + part_in[p][1, e, b].astype(f32)).astype(bf16)
            sigma = on_top(side_by_side(real, imag), side_by_side(-imag, real))
            both = wide_bare[e, b, pl.ds(0, size), :]
            product = matmul(both, sigma).astype(bf16)
            new = (both.astype(f32) + matmul(product, wide_bare[e, b])).astype(bf16)
            if p == passes - 1:
                out[0, 0, e, b] = new[:, :size]
                out[1, 0, e, b] = new[:, size:]
            else:
                real_current[p][e][b] = new[:, :size]
                imag_source[p + 1][e][1, b] = new[:, size:]
        if p < passes - 1:
            start(p + 1, RAW_NEXT, e)
            start(p + 1, RAW_PREV, e)
            start(p + 1, RAW_UP, e)
            start(p + 1, RAW_DOWN, e)

    for p in range(passes):
        imag_order = ends + middle if p == 0 else middle + ends
        share_order = middle + ends
        shares, done, sent = list(share_order), set(), set()

        def ready_parts():
            found = []
            for i in range(energies):
                if all(j in done for j in range(i + 1)):
                    found.append((0, i))
                if all(j in done for j in range(energies - 1 - i, energies)):
                    found.append((1, energies - 1 - i))
            return [item for item in found if item not in sent]

        def send_next_part():
            way_and_energy = ready_parts()[0]
            sent.add(way_and_energy)
            send_part(p, *way_and_energy)

        for e in imag_order:
            if p == 0 and e == imag_order[-1]:
                for _ in middle:
                    real_step(p, shares.pop(0))
            imag_step(p, e)
            done.add(e)
            if len(done) < energies:
                while ready_parts():
                    send_next_part()
        while ready_parts() or shares:
            if ready_parts():
                send_next_part()
            if shares and not (p == 0 and len(ready_parts()) % 2):
                real_step(p, shares.pop(0))
        for e in share_order:
            part_own[e] = part_of(e)
        for e in share_order:
            close_step(p, e)

    for p in range(passes):
        for kind in range(KINDS):
            def finish(p=p, kind=kind):
                for e in range(energies):
                    copy_of(p, kind, e).wait_send()

            guarded(sends_if(kind), finish)


def shards(mom_count, en_count, green, bare, coupling, occupation, mode_shift, mode_offset, mode_block):
    _, _, energies, blocks, size, _ = green.shape
    assert energies == REACH and coupling.shape[0] == MODES and MODES == REACH
    pair = (blocks, size, size)
    vmem = pltpu.VMEM
    smem = pltpu.SMEM
    scratch = [
        smem(occupation.shape, occupation.dtype),
        smem(mode_shift.shape, mode_shift.dtype),
        smem(mode_offset.shape, mode_offset.dtype),
        smem(mode_block.shape, mode_block.dtype),
        vmem(bare.shape, bf16),
        vmem(coupling.shape, bf16),
        [vmem(pair, bf16) for _ in range(energies)],
        vmem((MODES, size, size), bf16),
        vmem((MODES * size, size), bf16),
        vmem((3, 2 * size, size), bf16),
        vmem((energies, blocks, 2 * size, 2 * size), bf16),
        vmem((energies, MODES, blocks * size, size), bf16),
        vmem((energies, MODES) + pair, bf16),
        vmem((energies, MODES) + pair, bf16),
        vmem((energies, blocks * size, size), f32),
        vmem((energies, blocks * size, size), f32),
        [[vmem(pair, bf16) for _ in range(energies)] for _ in range(PASSES - 1)],
        [[vmem(pair, bf16) for _ in range(energies)] for _ in range(PASSES)],
        [[vmem(pair, bf16) for _ in range(energies)] for _ in range(PASSES)],
        [[vmem((3,) + pair, bf16) for _ in range(energies)] for _ in range(PASSES)],
        [vmem((2, energies) + pair, bf16) for _ in range(PASSES)],
        [vmem((2, energies) + pair, bf16) for _ in range(PASSES)],
        [vmem((2, energies) + pair, bf16) for _ in range(PASSES)],
        [vmem((2, energies) + pair, bf16) for _ in range(PASSES)],
        pltpu.SemaphoreType.DMA((PASSES, KINDS, energies)),
        pltpu.SemaphoreType.DMA((PASSES, KINDS, energies)),
        pltpu.SemaphoreType.DMA((2, energies)),
        pltpu.SemaphoreType.DMA((6,)),
    ]
    whole = pl.BlockSpec(memory_space=pltpu.VMEM)
    anywhere = pl.BlockSpec(memory_space=pl.ANY)
    return pl.pallas_call(
        functools.partial(kernel, mom_count, en_count, PASSES),
        out_shape=jax.ShapeDtypeStruct(green.shape, green.dtype),
        in_specs=[anywhere] * 7,
        out_specs=whole,
        scratch_shapes=scratch,
        compiler_params=pltpu.CompilerParams(collective_id=0, has_side_effects=True),
        name="born_passes",
    )(occupation, mode_shift, mode_offset, mode_block, green, bare, coupling)


def solution(mesh):
    spread = P(None, "mom", "en", None, None, None)
    return jax.shard_map(
        functools.partial(shards, mesh.shape["mom"], mesh.shape["en"]),
        mesh=mesh,
        in_specs=(spread, spread, P(), P(), P(), P(), P()),
        out_specs=spread,
        check_vma=False,
    )
```

```python
import functools

import jax
import jax.numpy as jnp
from jax import lax
from jax.experimental import pallas as pl
from jax.experimental.pallas import tpu as pltpu
from jax.sharding import PartitionSpec as P

MODES = 4
REACH = 4
PASSES = 2

RAW_UP, RAW_DOWN, RAW_NEXT, RAW_PREV, SHARE_NEXT, SHARE_PREV, PART_UP, PART_DOWN = range(8)
KINDS = 8

f32 = jnp.float32
bf16 = jnp.bfloat16


def matmul(left, right):
    return jnp.dot(left, right, preferred_element_type=f32)


def side_by_side(*parts):
    return parts[0] if len(parts) == 1 else jnp.concatenate(parts, axis=1)


def on_top(*parts):
    return parts[0] if len(parts) == 1 else jnp.concatenate(parts, axis=0)


def kernel(
    mom_count, en_count, passes,
    occupation_hbm, mode_shift_hbm, mode_offset_hbm, mode_block_hbm, green, bare_hbm, coupling_hbm,
    out,
    occupation, mode_shift, mode_offset, mode_block, bare, coupling, first_real,
    matrices, matrices_t, pair_t, wide_bare, real_coupled, below, above,
    share_own, part_own, real_current, low_rim, high_rim, imag_source,
    share_out, share_in, part_out, part_in, send_sem, recv_sem, green_sem, input_sem,
):
    energies = green.shape[2]
    blocks = green.shape[3]
    size = green.shape[4]
    k = lax.axis_index("mom")
    z = lax.axis_index("en")
    next_k = lax.rem(k + 1, mom_count)
    prev_k = lax.rem(k + mom_count - 1, mom_count)
    up_z = lax.rem(z + 1, en_count)
    down_z = lax.rem(z + en_count - 1, en_count)
    has_up = z < en_count - 1
    has_down = z > 0

    barrier = pltpu.get_barrier_semaphore()
    for other in (next_k, prev_k):
        pl.semaphore_signal(
            barrier, inc=1, device_id={"mom": other}, device_id_type=pl.DeviceIdType.MESH
        )

    @pl.when(has_up)
    def _():
        pl.semaphore_signal(
            barrier, inc=1, device_id={"en": up_z}, device_id_type=pl.DeviceIdType.MESH
        )

    @pl.when(has_down)
    def _():
        pl.semaphore_signal(
            barrier, inc=1, device_id={"en": down_z}, device_id_type=pl.DeviceIdType.MESH
        )

    middle = list(range(1, energies - 1))
    ends = [0, energies - 1]
    upward = list(range(energies))[::-1]
    downward = list(range(energies))

    real_fetch = [
        pltpu.make_async_copy(green.at[0, 0, e], first_real[e], green_sem.at[0, e])
        for e in range(energies)
    ]
    imag_fetch = [
        pltpu.make_async_copy(green.at[1, 0, e], imag_source[0][e].at[1], green_sem.at[1, e])
        for e in range(energies)
    ]
    pairs = (
        (coupling_hbm, coupling),
        (bare_hbm, bare),
        (occupation_hbm, occupation),
        (mode_shift_hbm, mode_shift),
        (mode_offset_hbm, mode_offset),
        (mode_block_hbm, mode_block),
    )
    input_fetch = [
        pltpu.make_async_copy(there, here, input_sem.at[i]) for i, (there, here) in enumerate(pairs)
    ]
    for e in ends + middle:
        imag_fetch[e].start()
        real_fetch[e].start()
    for fetch in input_fetch:
        fetch.start()

    pl.semaphore_wait(barrier, 2 + has_up.astype(jnp.int32) + has_down.astype(jnp.int32))

    def copy_of(p, kind, e):
        if kind == RAW_UP or kind == RAW_DOWN:
            source = first_real[e] if p == 0 else real_current[p - 1][e]
            target = low_rim[p][e] if kind == RAW_UP else high_rim[p][e]
        elif kind == RAW_NEXT or kind == RAW_PREV:
            source = imag_source[p][e].at[1]
            target = imag_source[p][e].at[2 if kind == RAW_NEXT else 0]
        elif kind == SHARE_NEXT or kind == SHARE_PREV:
            way = 1 if kind == SHARE_NEXT else 0
            source, target = share_out[p].at[way, e], share_in[p].at[way, e]
        else:
            way = 1 if kind == PART_UP else 0
            source, target = part_out[p].at[way, e], part_in[p].at[way, e]
        if kind in (RAW_NEXT, SHARE_NEXT):
            device = {"mom": next_k}
        elif kind in (RAW_PREV, SHARE_PREV):
            device = {"mom": prev_k}
        elif kind in (RAW_UP, PART_UP):
            device = {"en": up_z}
        else:
            device = {"en": down_z}
        return pltpu.make_async_remote_copy(
            src_ref=source,
            dst_ref=target,
            send_sem=send_sem.at[p, kind, e],
            recv_sem=recv_sem.at[p, kind, e],
            device_id=device,
            device_id_type=pl.DeviceIdType.MESH,
        )

    def guarded(condition, action):
        if condition is None:
            action()
        else:
            pl.when(condition)(action)

    def sends_if(kind):
        return {RAW_UP: has_up, PART_UP: has_up, RAW_DOWN: has_down, PART_DOWN: has_down}.get(kind)

    def receives_if(kind):
        return {RAW_UP: has_down, PART_UP: has_down, RAW_DOWN: has_up, PART_DOWN: has_up}.get(kind)

    def start(p, kind, e):
        guarded(sends_if(kind), lambda: copy_of(p, kind, e).start())

    waited = set()

    def arrived(p, kind, e):
        if (p, kind, e) not in waited:
            waited.add((p, kind, e))
            guarded(receives_if(kind), lambda: copy_of(p, kind, e).wait_recv())

    for i, e in enumerate(ends + middle):
        imag_fetch[e].wait()
        start(0, RAW_NEXT, e)
        start(0, RAW_PREV, e)
    for fetch in real_fetch:
        fetch.wait()
    for i in range(energies):
        start(0, RAW_UP, upward[i])
        start(0, RAW_DOWN, downward[i])

    @pl.when(jnp.logical_not(has_down))
    def _():
        for p in range(passes):
            for e in range(energies):
                low_rim[p][e][...] = jnp.zeros_like(low_rim[p][e])
            part_in[p][1] = jnp.zeros_like(part_in[p][1])

    @pl.when(jnp.logical_not(has_up))
    def _():
        for p in range(passes):
            for e in range(energies):
                high_rim[p][e][...] = jnp.zeros_like(high_rim[p][e])
            part_in[p][0] = jnp.zeros_like(part_in[p][0])

    for fetch in input_fetch:
        fetch.wait()

    weight, shift, picks = [], [], []
    for m in range(MODES):
        mode = jnp.int32(0)
        for j in range(1, MODES):
            mode = jnp.where(mode_offset[j] == m + 1, jnp.int32(j), mode)
        weight.append(occupation[mode])
        shift.append(mode_shift[mode])
        picks.append([mode_block[b, mode] for b in range(blocks)])
        matrix = coupling[mode]
        matrices[m] = matrix
        matrices_t[pl.ds(m * size, size), :] = matrix.astype(f32).T.astype(bf16)
    slot_of = []
    for q in (-1, 0, 1):
        slot = jnp.int32(0)
        for m in range(1, MODES):
            slot = jnp.where(shift[m] == q, jnp.int32(m), slot)
        slot_of.append(slot)
    extra = sum(range(MODES)) - slot_of[0] - slot_of[1] - slot_of[2]
    extra_shift = jnp.int32(0)
    for m in range(MODES):
        extra_shift = jnp.where(extra == m, shift[m], extra_shift)
    extra_t = matrices[extra].astype(f32).T
    for q in range(3):
        pair_t[q, pl.ds(0, size), :] = matrices[slot_of[q]].astype(f32).T.astype(bf16)
        kept = jnp.where(extra_shift == q - 1, 1.0, 0.0).astype(f32)
        pair_t[q, pl.ds(size, size), :] = (extra_t * kept).astype(bf16)

    for e in range(energies):
        for b in range(blocks):
            real, imag = bare[0, 0, e, b], bare[1, 0, e, b]
            wide_bare[e, b, pl.ds(0, size), :] = side_by_side(real, imag)
            wide_bare[e, b, pl.ds(size, size), :] = side_by_side(-imag, real)

    def real_at(p, e, pick):
        if e < 0:
            return low_rim[p][e + energies][pick]
        if e >= energies:
            return high_rim[p][e - energies][pick]
        return first_real[e][pick] if p == 0 else real_current[p - 1][e][pick]

    def imag_step(p, e):
        arrived(p, RAW_NEXT, e)
        arrived(p, RAW_PREV, e)
        for m in range(MODES):
            chosen = imag_source[p][e][shift[m] + 1]
            coupled = matmul(matrices[m], side_by_side(*[chosen[c] for c in range(blocks)]))
            lower = (weight[m] * coupled).astype(bf16)
            upper = ((weight[m] + 1.0) * coupled).astype(bf16)
            for c in range(blocks):
                below[e, m, c] = lower[:, c * size:(c + 1) * size]
                above[e, m, c] = upper[:, c * size:(c + 1) * size]

    def part_of(target):
        lower = [m for m in range(MODES) if 0 <= target - m - 1 < energies]
        upper = [m for m in range(MODES) if 0 <= target + m + 1 < energies]
        rows = []
        for b in range(blocks):
            terms = [below[target - m - 1, m, picks[m][b]] for m in lower]
            terms += [above[target + m + 1, m, picks[m][b]] for m in upper]
            rows.append(side_by_side(*terms))
        spans = [
            matrices_t[pl.ds(ms[0] * size, len(ms) * size), :] for ms in (lower, upper) if ms
        ]
        return matmul(on_top(*rows), on_top(*spans))

    def send_part(p, way, e):
        target = e + energies if way == 1 else e - energies
        part = part_of(target).astype(bf16)
        for b in range(blocks):
            part_out[p][way, e, b] = part[b * size:(b + 1) * size]
        start(p, PART_UP if way == 1 else PART_DOWN, e)

    def real_step(p, e):
        for m in range(MODES):
            for at in (e - m - 1, e + m + 1):
                if at < 0:
                    arrived(p, RAW_UP, at + energies)
                elif at >= energies:
                    arrived(p, RAW_DOWN, at - energies)
        for m in range(MODES):
            summed = []
            for b in range(blocks):
                low_side = real_at(p, e - m - 1, picks[m][b]).astype(f32)
                high_side = real_at(p, e + m + 1, picks[m][b]).astype(f32)
                mixed = weight[m] * low_side + (weight[m] + 1.0) * high_side
                summed.append(mixed.astype(bf16))
            coupled = matmul(matrices[m], side_by_side(*summed)).astype(bf16)
            for b in range(blocks):
                real_coupled[e, m, pl.ds(b * size, size), :] = coupled[:, b * size:(b + 1) * size]
        rest = real_coupled[e, extra]
        for q in (0, 2, 1):
            share = matmul(side_by_side(real_coupled[e, slot_of[q]], rest), pair_t[q])
            if q == 1:
                share_own[e] = share
            else:
                rounded = share.astype(bf16)
                way = 1 if q == 2 else 0
                for b in range(blocks):
                    share_out[p][way, e, b] = rounded[b * size:(b + 1) * size]
                start(p, SHARE_NEXT if way == 1 else SHARE_PREV, e)

    def close_step(p, e):
        for kind in (SHARE_NEXT, SHARE_PREV, PART_UP, PART_DOWN):
            arrived(p, kind, e)
        for b in range(blocks):
            rows = slice(b * size, (b + 1) * size)
            real = share_own[e, rows] + share_in[p][0, e, b].astype(f32)
            real = (real + share_in[p][1, e, b].astype(f32)).astype(bf16)
            imag = part_own[e, rows] + part_in[p][0, e, b].astype(f32)
            imag = (imag + part_in[p][1, e, b].astype(f32)).astype(bf16)
            sigma = on_top(side_by_side(real, imag), side_by_side(-imag, real))
            both = wide_bare[e, b, pl.ds(0, size), :]
            product = matmul(both, sigma).astype(bf16)
            new = (both.astype(f32) + matmul(product, wide_bare[e, b])).astype(bf16)
            if p == passes - 1:
                out[0, 0, e, b] = new[:, :size]
                out[1, 0, e, b] = new[:, size:]
            else:
                real_current[p][e][b] = new[:, :size]
                imag_source[p + 1][e][1, b] = new[:, size:]
        if p < passes - 1:
            start(p + 1, RAW_NEXT, e)
            start(p + 1, RAW_PREV, e)
            start(p + 1, RAW_UP, e)
            start(p + 1, RAW_DOWN, e)

    for p in range(passes):
        imag_order = ends + middle if p == 0 else middle + ends
        share_order = middle + ends
        shares, done, sent = list(share_order), set(), set()

        def ready_parts():
            found = []
            for i in range(energies):
                if all(j in done for j in range(i + 1)):
                    found.append((0, i))
                if all(j in done for j in range(energies - 1 - i, energies)):
                    found.append((1, energies - 1 - i))
            return [item for item in found if item not in sent]

        def send_next_part():
            way_and_energy = ready_parts()[0]
            sent.add(way_and_energy)
            send_part(p, *way_and_energy)

        for e in imag_order:
            if (p == 0 and e == imag_order[len(ends)]) or (p > 0 and e == imag_order[-1]):
                for _ in middle:
                    real_step(p, shares.pop(0))
            imag_step(p, e)
            done.add(e)
            if len(done) < energies:
                while ready_parts():
                    send_next_part()
        while ready_parts() or shares:
            if ready_parts():
                send_next_part()
            if shares and len(ready_parts()) % 2 == 0:
                real_step(p, shares.pop(0))
        for e in share_order:
            part_own[e] = part_of(e)
        for e in share_order:
            close_step(p, e)

    for p in range(passes):
        for kind in range(KINDS):
            def finish(p=p, kind=kind):
                for e in range(energies):
                    copy_of(p, kind, e).wait_send()

            guarded(sends_if(kind), finish)


def shards(mom_count, en_count, green, bare, coupling, occupation, mode_shift, mode_offset, mode_block):
    _, _, energies, blocks, size, _ = green.shape
    assert energies == REACH and coupling.shape[0] == MODES and MODES == REACH
    pair = (blocks, size, size)
    vmem = pltpu.VMEM
    smem = pltpu.SMEM
    scratch = [
        smem(occupation.shape, occupation.dtype),
        smem(mode_shift.shape, mode_shift.dtype),
        smem(mode_offset.shape, mode_offset.dtype),
        smem(mode_block.shape, mode_block.dtype),
        vmem(bare.shape, bf16),
        vmem(coupling.shape, bf16),
        [vmem(pair, bf16) for _ in range(energies)],
        vmem((MODES, size, size), bf16),
        vmem((MODES * size, size), bf16),
        vmem((3, 2 * size, size), bf16),
        vmem((energies, blocks, 2 * size, 2 * size), bf16),
        vmem((energies, MODES, blocks * size, size), bf16),
        vmem((energies, MODES) + pair, bf16),
        vmem((energies, MODES) + pair, bf16),
        vmem((energies, blocks * size, size), f32),
        vmem((energies, blocks * size, size), f32),
        [[vmem(pair, bf16) for _ in range(energies)] for _ in range(PASSES - 1)],
        [[vmem(pair, bf16) for _ in range(energies)] for _ in range(PASSES)],
        [[vmem(pair, bf16) for _ in range(energies)] for _ in range(PASSES)],
        [[vmem((3,) + pair, bf16) for _ in range(energies)] for _ in range(PASSES)],
        [vmem((2, energies) + pair, bf16) for _ in range(PASSES)],
        [vmem((2, energies) + pair, bf16) for _ in range(PASSES)],
        [vmem((2, energies) + pair, bf16) for _ in range(PASSES)],
        [vmem((2, energies) + pair, bf16) for _ in range(PASSES)],
        pltpu.SemaphoreType.DMA((PASSES, KINDS, energies)),
        pltpu.SemaphoreType.DMA((PASSES, KINDS, energies)),
        pltpu.SemaphoreType.DMA((2, energies)),
        pltpu.SemaphoreType.DMA((6,)),
    ]
    whole = pl.BlockSpec(memory_space=pltpu.VMEM)
    anywhere = pl.BlockSpec(memory_space=pltpu.HBM)
    return pl.pallas_call(
        functools.partial(kernel, mom_count, en_count, PASSES),
        out_shape=jax.ShapeDtypeStruct(green.shape, green.dtype),
        in_specs=[anywhere] * 7,
        out_specs=whole,
        scratch_shapes=scratch,
        compiler_params=pltpu.CompilerParams(
            collective_id=0, has_side_effects=True, vmem_limit_bytes=40 * 1024 * 1024
        ),
        name="born_passes",
    )(*[pltpu.with_memory_space_constraint(a, pltpu.HBM) for a in (occupation, mode_shift, mode_offset, mode_block, green, bare, coupling)])


def solution(mesh):
    spread = P(None, "mom", "en", None, None, None)
    return jax.shard_map(
        functools.partial(shards, mesh.shape["mom"], mesh.shape["en"]),
        mesh=mesh,
        in_specs=(spread, spread, P(), P(), P(), P(), P()),
        out_specs=spread,
        check_vma=False,
    )
```
